32 devices in a mesh: dp: 8 (over y, x, core), tensor: 4 (over z).
Axes of the slice: x: 2, y: 2, z: 4, core: 2. Of those that a mesh axis runs over, the one named last changes fastest.
Arguments:
- inputs: bfloat16 [2048, 2048], P('dp'), may hold values from -6 to 6
- ln_gain: float32 [2048], replicated, may hold values from 0.5 to 1.5
- ln_bias: float32 [2048], replicated, may hold values from -1.75 to 1.75
- w_qkv: bfloat16 [2048, 6144], P(None, 'tensor'), may hold values from -1 to 1
- b_qkv: float32 [6144], P('tensor'), may hold values from -1.75 to 1.75
- w_out: bfloat16 [2048, 2048], P('tensor'), may hold values from -0.75 to 0.75
- b_out: float32 [2048], replicated, may hold values from -1.75 to 1.75
- w_fc1: bfloat16 [2048, 8192], P(None, 'tensor'), may hold values from -0.125 to 0.125
- b_fc1: float32 [8192], P('tensor'), may hold values from -3 to 3
- w_fc2: bfloat16 [8192, 2048], P('tensor'), may hold values from -0.0625 to 0.0625
- b_fc2: float32 [2048], replicated, may hold values from -1.75 to 1.75
- cotangent: bfloat16 [2048, 2048], P('dp')
Outputs:
- output: bfloat16 [2048, 2048], P('dp')
- input_grad: float32 [2048, 2048], P('dp')
- grad_ln_gain: float32 [2048], replicated
- grad_ln_bias: float32 [2048], replicated
- grad_w_qkv: float32 [2048, 6144], P(None, 'tensor')
- grad_b_qkv: float32 [6144], P('tensor')
- grad_w_out: float32 [2048, 2048], P('tensor')
- grad_b_out: float32 [2048], replicated
- grad_w_fc1: float32 [2048, 8192], P(None, 'tensor')
- grad_b_fc1: float32 [8192], P('tensor')
- grad_w_fc2: float32 [8192, 2048], P('tensor')
- grad_b_fc2: float32 [2048], replicated
The draws below stay inside these ranges and needn't reach their ends.
All inputs are finite; a program needn't handle non-finite values.
Results may differ from the reference program's by a relative error of at most 0.02.
Values may be sent and summed in bfloat16 or wider, within the bound.
A program may use at most 320 MiB of HBM per device.

```python
import jax
import jax.numpy as jnp
from jax import lax

D = 2048
H = 32
HD = 64
ROT = 32
FF = 8192
SEQ = 256
TOKENS = 2048
N_DP = 8


def draw_inputs(key, part):
    own = jax.random.fold_in(key, 11)
    keys = jax.random.split(own, 1)
    values = jnp.clip(jax.random.normal(keys[0], (TOKENS, D), jnp.float32), -6.0, 6.0)
    return values.astype(jnp.bfloat16)


def draw_w_qkv(key, part):
    own = jax.random.fold_in(key, 23)
    keys = jax.random.split(own, 1)
    values = jnp.clip(jax.random.normal(keys[0], (D, H, 3, HD), jnp.float32), -5.0, 5.0) * D ** (-0.5)
    return values.reshape(D, 3 * H * HD).astype(jnp.bfloat16)


def draw_cotangent(key, part):
    rows = jnp.arange(TOKENS).astype(jnp.float32)[:, None] / TOKENS
    factor = 0.5 + rows
    base = jnp.clip(jax.random.normal(key, (TOKENS, D), jnp.float32), -5.0, 5.0)
    return (base * factor).astype(jnp.bfloat16)


def levels(own_key, shape, shards, low, high):
    def one(axis_at, shards_of):
        draws = jax.random.uniform(jax.random.fold_in(jax.random.fold_in(own_key, 6), axis_at), (shards_of,), jnp.float32, low / len(shards), high / len(shards))
        return jnp.repeat(jnp.exp(draws), shape[axis_at] // shards_of).reshape((-1,) + (1,) * (len(shape) - axis_at - 1))

    factor_of = one(*shards[0])
    for cut in shards[1:]:
        factor_of = factor_of * one(*cut)
    return factor_of


def bell_draw(rng, shape, width, limit, shards=(), kind=jnp.bfloat16):
    array = width * jax.random.normal(rng, shape, jnp.float32)
    if shards:
        array = array * levels(rng, shape, shards, -0.22, 0.18)
    return jnp.clip(array, -limit, limit).astype(kind)


def setup_inputs(seed: int = 0) -> dict:
    seeds = jax.random.split(jax.random.key(seed), 13)
    inputs = draw_inputs(jax.random.fold_in(seeds[12], 71), 0)
    ln_gain = jnp.clip(1.0 + 0.1 * jax.random.normal(seeds[1], (D,), jnp.float32), 0.5, 1.5)
    ln_bias = bell_draw(seeds[2], (D,), 0.3, 1.75, (), jnp.float32)
    w_qkv = draw_w_qkv(jax.random.fold_in(seeds[12], 71), 0)
    b_qkv = bell_draw(seeds[4], (3 * H * HD,), 0.3, 1.75, ((0, 4),), jnp.float32)
    w_out = bell_draw(seeds[5], (H * HD, D), HD ** -0.5, 0.75, ((0, 4),))
    b_out = bell_draw(seeds[6], (D,), 0.3, 1.75, (), jnp.float32)
    w_fc1 = bell_draw(seeds[7], (D, FF), D ** -0.5, 0.125, ((1, 4),))
    b_fc1 = bell_draw(seeds[8], (FF,), 0.5, 3.0, ((0, 4),), jnp.float32)
    w_fc2 = bell_draw(seeds[9], (FF, D), FF ** -0.5, 0.0625, ((0, 4),))
    b_fc2 = bell_draw(seeds[10], (D,), 0.3, 1.75, (), jnp.float32)
    cotangent = draw_cotangent(jax.random.fold_in(seeds[12], 71), 0)
    return {"inputs": inputs, "ln_gain": ln_gain, "ln_bias": ln_bias, "w_qkv": w_qkv, "b_qkv": b_qkv, "w_out": w_out, "b_out": b_out, "w_fc1": w_fc1, "b_fc1": b_fc1, "w_fc2": w_fc2, "b_fc2": b_fc2, "cotangent": cotangent}


EPS = 1e-05
GELU_C = 0.7978845608028654
GELU_A = 0.044715

def gelu(argument):
    inner = GELU_C * (argument + GELU_A * argument * argument * argument)
    return 0.5 * argument * (1.0 + jnp.tanh(inner))

def gelu_slope(argument):
    tangent = jnp.tanh(GELU_C * (argument + GELU_A * argument * argument * argument))
    return 0.5 * (1.0 + tangent) + 0.5 * argument * (1.0 - tangent * tangent) * GELU_C * (1.0 + 3.0 * GELU_A * argument * argument)

def rotary_tables(length):
    position = jnp.arange(length).astype(jnp.float32)
    freqs = 10000.0 ** (-(jnp.arange(ROT // 2).astype(jnp.float32) * 2.0 / ROT))
    angles = position[:, None] * freqs[None, :]
    return (jnp.cos(angles)[:, None, :], jnp.sin(angles)[:, None, :])

def rotate(tensor, cosine, sine):
    first = tensor[..., :ROT // 2]
    second = tensor[..., ROT // 2:ROT]
    return jnp.concatenate([first * cosine - second * sine, second * cosine + first * sine, tensor[..., ROT:]], axis=-1)

def unrotate(grad, cosine, sine):
    first = grad[..., :ROT // 2]
    second = grad[..., ROT // 2:ROT]
    return jnp.concatenate([first * cosine + second * sine, second * cosine - first * sine, grad[..., ROT:]], axis=-1)

def probabilities(query_rot, key_rot, logsum):
    length = query_rot.shape[0]
    scores = jnp.einsum('qhd,khd->hqk', query_rot.astype(jnp.float32), key_rot.astype(jnp.float32)) * HD ** (-0.5)
    causal = jnp.arange(length)[:, None] >= jnp.arange(length)[None, :]
    scores = jnp.where(causal[None], scores, -1e+30)
    if logsum is None:
        top = lax.optimization_barrier(jnp.max(scores, -1, keepdims=True))
        logsum = top + jnp.log(lax.optimization_barrier(jnp.sum(jnp.exp(scores - top), -1, keepdims=True)))
    return (jnp.exp(scores - logsum), logsum)

def forward(x_seq, ln_gain, ln_bias, w_qkv, b_qkv, w_out, w_fc1, b_fc1, w_fc2, cosine, sine):
    length = x_seq.shape[0]
    heads = w_out.shape[0] // HD
    widened = x_seq.astype(jnp.float32)
    average = lax.optimization_barrier(jnp.mean(widened, -1, keepdims=True))
    centered = widened - average
    inv_std = lax.rsqrt(lax.optimization_barrier(jnp.mean(centered * centered, -1, keepdims=True)) + EPS)
    normed_hat = centered * inv_std
    normed = (normed_hat * ln_gain + ln_bias).astype(jnp.bfloat16)
    projected = (jnp.dot(normed, w_qkv, preferred_element_type=jnp.float32) + b_qkv).reshape(length, heads, 3, HD)
    query_rot = rotate(projected[:, :, 0], cosine, sine).astype(jnp.bfloat16)
    key_rot = rotate(projected[:, :, 1], cosine, sine).astype(jnp.bfloat16)
    value_bf = projected[:, :, 2].astype(jnp.bfloat16)
    probs, logsum = probabilities(query_rot, key_rot, None)
    prob_bf = probs.astype(jnp.bfloat16)
    attended = jnp.einsum('hqk,khd->qhd', prob_bf.astype(jnp.float32), value_bf.astype(jnp.float32))
    attended = attended.astype(jnp.bfloat16).reshape(length, heads * HD)
    hidden_pre = jnp.dot(normed, w_fc1, preferred_element_type=jnp.float32) + b_fc1
    activated = gelu(hidden_pre).astype(jnp.bfloat16)
    partial_value = jnp.dot(attended, w_out, preferred_element_type=jnp.float32) + jnp.dot(activated, w_fc2, preferred_element_type=jnp.float32)
    saved = (normed_hat, inv_std, normed, query_rot, key_rot, value_bf, logsum, attended, hidden_pre, activated)
    return (partial_value, saved)

def backward(dy_bf, saved, w_qkv, w_out, w_fc1, w_fc2, cosine, sine):
    normed_hat, inv_std, normed, query_rot, key_rot, value_bf, logsum, attended, hidden_pre, activated = saved
    length = dy_bf.shape[0]
    heads = w_out.shape[0] // HD
    g_w2 = jnp.dot(activated.T, dy_bf, preferred_element_type=jnp.float32)
    dhidden = jnp.dot(dy_bf, w_fc2.T, preferred_element_type=jnp.float32) * gelu_slope(hidden_pre)
    g_b1 = lax.optimization_barrier(jnp.sum(dhidden, 0))
    dhidden_bf = dhidden.astype(jnp.bfloat16)
    g_w1 = jnp.dot(normed.T, dhidden_bf, preferred_element_type=jnp.float32)
    dnormed = jnp.dot(dhidden_bf, w_fc1.T, preferred_element_type=jnp.float32)
    g_wout = jnp.dot(attended.T, dy_bf, preferred_element_type=jnp.float32)
    dattn_bf = jnp.dot(dy_bf, w_out.T, preferred_element_type=jnp.float32).astype(jnp.bfloat16).reshape(length, heads, HD)
    probs, logsum = probabilities(query_rot, key_rot, logsum)
    prob_bf = probs.astype(jnp.bfloat16)
    delta = lax.optimization_barrier(jnp.sum(dattn_bf.astype(jnp.float32) * attended.reshape(length, heads, HD).astype(jnp.float32), -1))
    dprob = jnp.einsum('qhd,khd->hqk', dattn_bf.astype(jnp.float32), value_bf.astype(jnp.float32))
    dscore_bf = (probs * (dprob - jnp.transpose(delta)[:, :, None]) * HD ** (-0.5)).astype(jnp.bfloat16)
    dquery = jnp.einsum('hqk,khd->qhd', dscore_bf.astype(jnp.float32), key_rot.astype(jnp.float32))
    dkey = jnp.einsum('hqk,qhd->khd', dscore_bf.astype(jnp.float32), query_rot.astype(jnp.float32))
    dvalue = jnp.einsum('hqk,qhd->khd', prob_bf.astype(jnp.float32), dattn_bf.astype(jnp.float32))
    dproj = jnp.stack([unrotate(dquery, cosine, sine), unrotate(dkey, cosine, sine), dvalue], axis=2).reshape(length, heads * 3 * HD)
    g_bqkv = lax.optimization_barrier(jnp.sum(dproj, 0))
    dproj_bf = dproj.astype(jnp.bfloat16)
    g_wqkv = jnp.dot(normed.T, dproj_bf, preferred_element_type=jnp.float32)
    dnormed = dnormed + jnp.dot(dproj_bf, w_qkv.T, preferred_element_type=jnp.float32)
    return (dnormed, (g_wqkv, g_bqkv, g_wout, g_w1, g_b1, g_w2))

def norm_back(dnormed, dy_bf, normed_hat, inv_std, ln_gain):
    g_gain = lax.optimization_barrier(jnp.sum(dnormed * normed_hat, 0))
    g_bias = lax.optimization_barrier(jnp.sum(dnormed, 0))
    scaled = dnormed * ln_gain
    inner = scaled - lax.optimization_barrier(jnp.mean(scaled, -1, keepdims=True)) - normed_hat * lax.optimization_barrier(jnp.mean(scaled * normed_hat, -1, keepdims=True))
    return (dy_bf.astype(jnp.float32) + inv_std * inner, g_gain, g_bias)

def reference(inputs, ln_gain, ln_bias, w_qkv, b_qkv, w_out, b_out, w_fc1, b_fc1, w_fc2, b_fc2, cotangent):
    cosine, sine = rotary_tables(SEQ)
    seq_inputs = inputs.reshape(N_DP, SEQ, D)
    seq_cots = cotangent.reshape(N_DP, SEQ, D)

    def one_sequence(carry, pair):
        x_seq, dy_seq = pair
        partial_value, saved = forward(x_seq, ln_gain, ln_bias, w_qkv, b_qkv, w_out, w_fc1, b_fc1, w_fc2, cosine, sine)
        output = (x_seq.astype(jnp.float32) + partial_value + b_out + b_fc2).astype(jnp.bfloat16)
        dnormed, grads = backward(dy_seq, saved, w_qkv, w_out, w_fc1, w_fc2, cosine, sine)
        dx_seq, g_gain, g_bias = norm_back(dnormed, dy_seq, saved[0], saved[1], ln_gain)
        g_bout = lax.optimization_barrier(jnp.sum(dy_seq.astype(jnp.float32), 0))
        terms = (g_gain, g_bias) + grads + (g_bout,)
        carry = tuple((total + term for total, term in zip(carry, terms)))
        return (carry, (output, dx_seq))
    start = (jnp.zeros((D,), jnp.float32), jnp.zeros((D,), jnp.float32), jnp.zeros((D, 3 * H * HD), jnp.float32), jnp.zeros((3 * H * HD,), jnp.float32), jnp.zeros((H * HD, D), jnp.float32), jnp.zeros((D, FF), jnp.float32), jnp.zeros((FF,), jnp.float32), jnp.zeros((FF, D), jnp.float32), jnp.zeros((D,), jnp.float32))
    totals, (outputs, dxs) = lax.scan(one_sequence, start, (seq_inputs, seq_cots))
    g_gain, g_bias, g_wqkv, g_bqkv, g_wout, g_w1, g_b1, g_w2, g_bout = totals
    return (outputs.reshape(TOKENS, D), dxs.reshape(TOKENS, D), g_gain, g_bias, g_wqkv, g_bqkv, g_wout, g_bout, g_w1, g_b1, g_w2, g_bout)
```

```python
import jax
import jax.numpy as jnp
from jax import lax
from jax.sharding import PartitionSpec as P

HD = 64
ROT = 32
EPS = 1e-05
GELU_C = 0.7978845608028654
GELU_A = 0.044715
BF = jnp.bfloat16
F32 = jnp.float32


def gelu_pair(u):
    tangent = jnp.tanh(GELU_C * (u + GELU_A * u * u * u))
    act = 0.5 * u * (1.0 + tangent)
    slope = 0.5 * (1.0 + tangent) + 0.5 * u * (1.0 - tangent * tangent) * GELU_C * (
        1.0 + 3.0 * GELU_A * u * u
    )
    return act, slope


def rotary_tables(length):
    position = jnp.arange(length).astype(F32)
    freqs = 10000.0 ** (-(jnp.arange(ROT // 2).astype(F32) * 2.0 / ROT))
    angles = position[:, None] * freqs[None, :]
    return (jnp.cos(angles)[:, None, :], jnp.sin(angles)[:, None, :])


def rotate(tensor, cosine, sine):
    first = tensor[..., : ROT // 2]
    second = tensor[..., ROT // 2 : ROT]
    return jnp.concatenate(
        [first * cosine - second * sine, second * cosine + first * sine, tensor[..., ROT:]], axis=-1
    )


def dot(a, b):
    return jnp.dot(a, b, preferred_element_type=F32)


def dot_nt(a, b):
    return lax.dot_general(a, b, (((1,), (1,)), ((), ())), preferred_element_type=F32)


def dot_tn(a, b):
    return lax.dot_general(a, b, (((0,), (0,)), ((), ())), preferred_element_type=F32)


def layer_norm(x, ln_gain, ln_bias):
    widened = x.astype(F32)
    average = jnp.mean(widened, -1, keepdims=True)
    centered = widened - average
    inv_std = lax.rsqrt(jnp.mean(centered * centered, -1, keepdims=True) + EPS)
    xhat = centered * inv_std
    return (xhat * ln_gain + ln_bias).astype(BF), xhat, inv_std


def attention(proj, dattn, length):
    rows = proj.shape[0]
    seqs = rows // length
    heads = dattn.shape[1] // HD
    cosine, sine = rotary_tables(length)
    projected = proj.reshape(seqs, length, heads, 3, HD)
    query = rotate(projected[:, :, :, 0], cosine, sine).astype(BF)
    key = rotate(projected[:, :, :, 1], cosine, sine).astype(BF)
    value = projected[:, :, :, 2].astype(BF)
    dattn = dattn.astype(BF).reshape(seqs, length, heads, HD)
    scores = jnp.einsum("sqhd,skhd->shqk", query, key, preferred_element_type=F32) * HD ** (-0.5)
    causal = jnp.arange(length)[:, None] >= jnp.arange(length)[None, :]
    scores = jnp.where(causal, scores, -1e30)
    top = jnp.max(scores, -1, keepdims=True)
    expo = jnp.exp(scores - top)
    probs = expo / jnp.sum(expo, -1, keepdims=True)
    prob_bf = probs.astype(BF)
    attended = jnp.einsum("shqk,skhd->sqhd", prob_bf, value, preferred_element_type=F32).astype(BF)
    delta = jnp.sum(dattn.astype(F32) * attended.astype(F32), -1)
    dprob = jnp.einsum("sqhd,skhd->shqk", dattn, value, preferred_element_type=F32)
    dscore = (probs * (dprob - jnp.swapaxes(delta, 1, 2)[..., None]) * HD ** (-0.5)).astype(BF)
    dquery = jnp.einsum("shqk,skhd->sqhd", dscore, key, preferred_element_type=F32)
    dkey = jnp.einsum("shqk,sqhd->skhd", dscore, query, preferred_element_type=F32)
    dvalue = jnp.einsum("shqk,sqhd->skhd", prob_bf, dattn, preferred_element_type=F32)
    dproj = jnp.stack(
        [rotate(dquery, cosine, -sine), rotate(dkey, cosine, -sine), dvalue], axis=3
    ).reshape(rows, heads * 3 * HD)
    return attended.reshape(rows, heads * HD), dproj.astype(BF), jnp.sum(dproj, 0)


def per_device(
    inputs, ln_gain, ln_bias, w_qkv, b_qkv, w_out, b_out, w_fc1, b_fc1, w_fc2, b_fc2, cotangent
):
    length = inputs.shape[0]
    n_dp = lax.axis_size("dp")
    n_tp = lax.axis_size("tensor")
    chips = n_dp // 2
    bits = chips.bit_length() - 1
    core = lax.axis_index("dp") % 2

    def hop(array, bit):
        perm = [(i, i ^ (2 << (bit if i % 2 == 0 else bits - 1 - bit))) for i in range(n_dp)]
        return lax.ppermute(array, "dp", perm)

    def sibling(array):
        return lax.ppermute(array, "dp", [(i, i ^ 1) for i in range(n_dp)])

    def half(array, axis):
        size = array.shape[axis] // 2
        return lax.dynamic_slice_in_dim(array, core * size, size, axis)

    def gather(array):
        got = {0: array}
        for mask in range(1, chips):
            low = (mask & -mask).bit_length() - 1
            got[mask] = hop(got[mask & (mask - 1)], low)
        return [jnp.concatenate([got[m], sibling(got[m])]) for m in range(chips)]

    xs = gather(inputs)
    gs = gather(cotangent)
    wq, bq = half(w_qkv, 1), half(b_qkv, 0)
    wo = half(w_out, 0)
    w1, b1 = half(w_fc1, 1), half(b_fc1, 0)
    w2 = half(w_fc2, 0)

    normed_all, act_all, dhid_all, att_all, dproj_all = [], [], [], [], []
    g_b1 = g_bqkv = 0.0
    for m in range(chips):
        x, g = xs[m], gs[m]
        normed, xhat, inv_std = layer_norm(x, ln_gain, ln_bias)
        hpre = dot(normed, w1) + b1
        act, slope = gelu_pair(hpre)
        act = act.astype(BF)
        dhid = dot_nt(g, w2) * slope
        g_b1 = g_b1 + jnp.sum(dhid, 0)
        dhid = dhid.astype(BF)
        att, dproj, gb = attention(dot(normed, wq) + bq, dot_nt(g, wo), length)
        g_bqkv = g_bqkv + gb
        if m == 0:
            part_out = dot(att, wo) + dot(act, w2)
            part_dn = dot_nt(dhid, w1) + dot_nt(dproj, wq)
            xhat_own, inv_own = xhat[:length], inv_std[:length]
        normed_all.append(normed)
        act_all.append(act)
        dhid_all.append(dhid)
        att_all.append(att)
        dproj_all.append(dproj)

    def reduce_tensor(part):
        own = part[:length] + sibling(part[length:].astype(BF)).astype(F32)
        own = own.astype(BF)
        index = lax.axis_index("tensor")
        steps = n_tp.bit_length() - 1
        held = own
        for s in range(steps):
            rows = held.shape[0] // 2
            bit = (index >> s) & 1
            keep = jnp.where(bit == 0, held[:rows], held[rows:])
            send = jnp.where(bit == 0, held[rows:], held[:rows])
            came = lax.ppermute(send, "tensor", [(i, i ^ (1 << s)) for i in range(n_tp)])
            held = (keep.astype(F32) + came.astype(F32)).astype(BF)
        for s in reversed(range(steps)):
            bit = (index >> s) & 1
            came = lax.ppermute(held, "tensor", [(i, i ^ (1 << s)) for i in range(n_tp)])
            held = jnp.where(
                bit == 0, jnp.concatenate([held, came]), jnp.concatenate([came, held])
            )
        return held.astype(F32)

    total = reduce_tensor(part_out)
    output = (inputs.astype(F32) + total + b_out + b_fc2).astype(BF)
    dnormed = reduce_tensor(part_dn)
    norms = jnp.stack([jnp.sum(dnormed * xhat_own, 0), jnp.sum(dnormed, 0)])
    scaled = dnormed * ln_gain
    inner = (
        scaled
        - jnp.mean(scaled, -1, keepdims=True)
        - xhat_own * jnp.mean(scaled * xhat_own, -1, keepdims=True)
    )
    input_grad = cotangent.astype(F32) + inv_own * inner
    for bit in range(bits + 1):
        norms = norms + lax.ppermute(norms, "dp", [(i, i ^ (1 << bit)) for i in range(n_dp)])

    normed_all = jnp.concatenate(normed_all)
    g_all = jnp.concatenate(gs)
    g_bout = jnp.sum(g_all.astype(F32), 0)

    def both_halves(own, axis):
        own = own.astype(BF)
        came = sibling(own)
        return jnp.where(
            core == 0,
            jnp.concatenate([own, came], axis),
            jnp.concatenate([came, own], axis),
        ).astype(F32)

    def both_bias(own):
        came = sibling(own)
        return jnp.where(core == 0, jnp.concatenate([own, came]), jnp.concatenate([came, own]))

    g_w2 = both_halves(dot_tn(jnp.concatenate(act_all), g_all), 0)
    g_w1 = both_halves(dot_tn(normed_all, jnp.concatenate(dhid_all)), 1)
    g_wout = both_halves(dot_tn(jnp.concatenate(att_all), g_all), 0)
    g_wqkv = both_halves(dot_tn(normed_all, jnp.concatenate(dproj_all)), 1)
    return (
        output,
        input_grad,
        norms[0],
        norms[1],
        g_wqkv,
        both_bias(g_bqkv),
        g_wout,
        g_bout,
        g_w1,
        both_bias(g_b1),
        g_w2,
        g_bout,
    )


def solution(mesh):
    placed = (
        P("dp", None),
        P(),
        P(),
        P(None, "tensor"),
        P("tensor"),
        P("tensor", None),
        P(),
        P(None, "tensor"),
        P("tensor"),
        P("tensor", None),
        P(),
        P("dp", None),
    )
    return jax.shard_map(
        per_device,
        mesh=mesh,
        in_specs=placed,
        out_specs=(
            P("dp", None),
            P("dp", None),
            P(),
            P(),
            P(None, "tensor"),
            P("tensor"),
            P("tensor", None),
            P(),
            P(None, "tensor"),
            P("tensor"),
            P("tensor", None),
            P(),
        ),
        check_vma=False,
    )
```
